32 devices in a mesh: temp: 8 (over y, x, core), bond: 4 (over z).
Axes of the slice: x: 2, y: 2, z: 4, core: 2. Of those that a mesh axis runs over, the one named last changes fastest.
Arguments:
- tensor: float32 [512, 4096], P(('temp', 'bond')), parts along dimension 0, may hold values from -6 to 6
- isometries: float32 [24, 64, 4096], P('temp', 'bond'), parts along dimension 0, may hold values from -0.09375 to 0.09375
Outputs:
- final_tensor: float32 [512, 4096], P(('temp', 'bond')), parts along dimension 0
- log_density: float32 [8], P('temp'), parts along dimension 0
The draws below stay inside these ranges and needn't reach their ends.
There are 8 independent parts, one for each index of `temp`. The reference program is written for one: setup_inputs(seed, part) draws one part's arguments, and reference() takes and returns one part's arrays. A program takes and returns all parts, laid end to end along the dimension named above; each array names one. Nothing has to cross between parts.
All inputs are finite; a program needn't handle non-finite values. Where the reference program divides by a largest or mean magnitude, that divisor is 1e-20 or more.
Results may differ from the reference program's by a relative error of at most 0.00027.
Values sent between devices are 32-bit elements; how exact they have to be, the bound alone decides.
No kernel may reach another device: no remote copies, remote signals or barrier semaphores. Data moves between devices by JAX's collectives and lax.ppermute only.
A program may use at most 128 MiB of HBM per device.

```python
import jax
import jax.numpy as jnp
from jax import lax

CHI = 64
LEVELS = 3


def shard_levels(rng, shape, cuts, low, high):
    factor_of, own = 1.0, jax.random.fold_in(rng, 6)
    for position, shards_of in cuts:
        steps = jnp.exp(jax.random.uniform(jax.random.fold_in(own, position), (shards_of,), jnp.float32, low / len(cuts), high / len(cuts)))
        factor_of = factor_of * jnp.repeat(steps, shape[position] // shards_of).reshape([-1 if axis == position else 1 for axis in range(len(shape))])
    return factor_of


def gaussian(key, extent, spread, reach, split=(), held_as=jnp.bfloat16):
    result = jax.random.normal(key, extent, jnp.float32) * spread
    if len(split) > 0:
        result = shard_levels(key, extent, split, -0.22, 0.18) * result
    return jnp.clip(result, min=-reach, max=reach).astype(held_as)


def setup_inputs(seed: int = 0, part: int = 0) -> dict:
    streams_of = jax.random.split(jax.random.key(seed), 3)
    part_keys = jax.random.split(jax.random.fold_in(streams_of[2], part), 3)
    tensor = gaussian(part_keys[0], (CHI, CHI * CHI), 1.0, 6.0, ((0, 4),), jnp.float32)
    isometries = gaussian(part_keys[1], (LEVELS, CHI, CHI * CHI), (CHI * CHI) ** -0.5, 0.09375, ((1, 4),), jnp.float32)
    return {"tensor": tensor, "isometries": isometries}


PRECISE = lax.Precision.HIGHEST
EPSILON = 1e-6


def unpack(flat):
    return flat.reshape(CHI, CHI, CHI).transpose(1, 2, 0)


def reference(tensor, isometries):
    log_density = jnp.zeros((1,), jnp.float32)
    current_flat = tensor
    for section_idx in range(LEVELS):
        current = unpack(current_flat)
        isometry = isometries[section_idx].reshape(CHI, CHI, CHI)
        inner_sum = jnp.einsum('bct,nst->nbcs', current, isometry, precision=PRECISE)
        summed = jnp.einsum('abs,nbcs->nac', current, inner_sum, precision=PRECISE)
        largest = jnp.max(jnp.abs(summed)) + EPSILON
        current_flat = summed.reshape(CHI, CHI * CHI) / largest
        log_density = log_density + jnp.log(largest) * (0.5 ** (section_idx + 1))
    return current_flat, log_density
```

```python
import functools

import jax
import jax.numpy as jnp
from jax import lax
from jax.experimental import pallas as pl
from jax.experimental.pallas import tpu as pltpu
from jax.sharding import PartitionSpec as P

EPSILON = 1e-06
LANES = 128
PITCH = 72
BF16 = jnp.bfloat16
F32 = jnp.float32


def pieces_of(own, parts):
    if parts == 4:
        far = lax.ppermute(own, "bond", [(0, 2), (2, 0), (1, 3), (3, 1)])
        near = lax.ppermute(own, "bond", [(0, 1), (1, 0), (2, 3), (3, 2)])
        middle = lax.ppermute(own, "bond", [(1, 2), (2, 1)])
        relayed = lax.ppermute(far, "bond", [(1, 0), (2, 3)])
        return [own, near, far, middle, relayed], lambda me: [me, me ^ 1, me ^ 2, me ^ 3, me ^ 3]
    return [lax.all_gather(own, "bond", axis=0, tiled=True)], lambda me: [0]


def level_kernel(count, sources, scaled, last, rows, width, *refs):
    pieces = refs[:count]
    u_ref, out_ref, largest_ref, peak_ref = refs[count : count + 4]
    whole, stacked, turned, factor, placed = refs[count + 4 :]
    held = pieces[0].shape[0]
    pairs = width // 2
    cells = width * width
    me = lax.axis_index("bond")
    found = sources(me)
    if scaled:
        largest = jnp.max(pieces[0][:, cells:])
        for piece in pieces[1:]:
            largest = jnp.maximum(largest, jnp.max(piece[:, cells:]))
        largest = jnp.full((8, LANES), largest, F32) + EPSILON
        largest_ref[...] = largest
        inverse = (1.0 / largest)[0:1, :]
    else:
        largest_ref[...] = jnp.ones((8, LANES), F32)
        inverse = None
    for j in range(count):
        start = pl.multiple_of(found[j] * held, 8)
        if j == count - 2 and count == 5:
            continue
        for x in range(pairs):
            value = pieces[j][:, x * LANES : (x + 1) * LANES]
            if j == count - 1 and count == 5:
                value = value + pieces[j - 1][:, x * LANES : (x + 1) * LANES]
            if scaled:
                value = value * inverse
            whole[pl.ds(start, held), x * LANES : (x + 1) * LANES] = value

    for x in range(pairs):
        lanes = slice(x * LANES, (x + 1) * LANES)
        value = whole[:, lanes]
        high = value.astype(BF16)
        high_wide = high.astype(F32)
        low = (value - high_wide).astype(BF16)
        stacked[0:width, lanes] = high
        stacked[width : 2 * width, lanes] = low
        stacked[2 * width : 3 * width, lanes] = high
        both = jnp.concatenate([high_wide, low.astype(F32)], axis=0).T
        turned[pl.ds(x, width, stride=PITCH), :] = both[:width]
        turned[pl.ds(pairs + x, width, stride=PITCH), :] = both[width:]

    groups = pairs // 4
    for g in range(groups):
        blocks = []
        for i in range(4):
            b = 2 * (4 * g + i)
            upper = turned[b * PITCH : b * PITCH + width, :].astype(BF16)
            lower = turned[(b + 1) * PITCH : (b + 1) * PITCH + width, :].astype(BF16)
            blocks.append(jnp.concatenate([upper, lower], axis=0))
        highs = [
            jnp.concatenate([blocks[i][:, :width], blocks[i + 1][:, :width]], axis=1)
            for i in (0, 2)
        ]
        factor[:, g * 768 : (g + 1) * 768] = jnp.concatenate(blocks + highs, axis=1)

    low_half = lax.broadcasted_iota(jnp.int32, (pairs, LANES), 1) < width

    def first(q, g):
        u = u_ref[0, pl.ds(pl.multiple_of(q * 4 * width, 4 * width), 4 * width), :]
        return jnp.dot(u, stacked[:, g * 512 : (g + 1) * 512], preferred_element_type=F32)

    def second(inner, g):
        high = inner.astype(BF16)
        low = (inner - high.astype(F32)).astype(BF16)

        def block(array, i):
            return jnp.concatenate(
                [array[n * width : (n + 1) * width, i * LANES : (i + 1) * LANES] for n in range(4)],
                axis=1,
            )

        highs = [block(high, i) for i in range(4)]
        lows = [block(low, i) for i in range(4)]
        weights = jnp.concatenate([h for h in highs for _ in range(2)] + lows, axis=0)
        return jnp.dot(
            factor[:, g * 768 : (g + 1) * 768], weights, preferred_element_type=F32
        )

    def quad(q, peak):
        total = None
        inner = first(q, 0)
        for g in range(groups):
            ahead = first(q, g + 1) if g + 1 < groups else None
            update = second(inner, g)
            total = update if total is None else total + update
            inner = ahead
        for n in range(4):
            part = total[:, n * LANES : (n + 1) * LANES]
            even0, odd0, even1, odd1 = (part[r * pairs : (r + 1) * pairs] for r in range(4))
            kept = jnp.where(low_half, even0, odd1)
            moved = jnp.where(low_half, odd0, even1)
            value = kept + pltpu.roll(moved, width, 1)
            peak = jnp.maximum(peak, jnp.abs(value))
            at = (q // 2) * (8 * pairs) + (q % 2) * 4 + n
            placed[pl.ds(at, pairs, stride=8), :] = value
        return peak

    peak = lax.fori_loop(0, rows // 4, quad, jnp.zeros((pairs, LANES), F32))
    tall = min(rows, 8)
    for h in range(rows // tall):
        for x in range(pairs):
            at = (h * pairs + x) * 8
            out_ref[h * tall : (h + 1) * tall, x * LANES : (x + 1) * LANES] = placed[at : at + tall, :]
    highest = jnp.max(peak)
    peak_ref[...] = jnp.full((8, LANES), highest, F32)
    if not last:
        out_ref[:, cells:] = jnp.full((rows, LANES), highest, F32)


def level(own, isometry, section, parts, scaled, last):
    arrays, sources = pieces_of(own, parts)
    count = len(arrays)
    rows, width = own.shape[0], own.shape[0] * parts
    cells = width * width
    span = cells if last else cells + LANES
    body = functools.partial(level_kernel, count, sources, scaled, last, rows, width)
    full = lambda shape: pl.BlockSpec(shape, lambda i: (0, 0))
    return pl.pallas_call(
        body,
        grid=(1,),
        in_specs=[full(a.shape) for a in arrays]
        + [pl.BlockSpec((1,) + isometry.shape[1:], lambda i: (section, 0, 0))],
        out_specs=[full((rows, span)), full((8, LANES)), full((8, LANES))],
        out_shape=[
            jax.ShapeDtypeStruct((rows, span), F32),
            jax.ShapeDtypeStruct((8, LANES), F32),
            jax.ShapeDtypeStruct((8, LANES), F32),
        ],
        scratch_shapes=[
            pltpu.VMEM((width, cells), F32),
            pltpu.VMEM((3 * width, cells), BF16),
            pltpu.VMEM((width * PITCH, LANES), F32),
            pltpu.VMEM((2 * width, 96 * width), BF16),
            pltpu.VMEM((max(rows, 8) * width // 2, LANES), F32),
        ],
        compiler_params=pltpu.CompilerParams(vmem_limit_bytes=48 * 1024 * 1024),
        name="level",
    )(*arrays, isometry)


def finish_kernel(sections, own_ref, peak_ref, *refs):
    scales = refs[: sections - 1]
    peaks = refs[sections - 1 : -2]
    out_ref, log_ref = refs[-2:]
    largest = peak_ref[...]
    for peak in peaks:
        largest = jnp.maximum(largest, peak[...])
    largest = largest + EPSILON
    log_density = jnp.log(largest) * 0.5**sections
    for k, scale in enumerate(scales):
        log_density = log_density + jnp.log(scale[...]) * 0.5 ** (k + 1)
    log_ref[...] = log_density
    out_ref[...] = own_ref[...] / largest[0:1, 0:1]


def on_device(tensor, isometries):
    parts = lax.axis_size("bond")
    sections = isometries.shape[0]
    rows = tensor.shape[0]
    width = rows * parts
    flat = isometries.reshape(sections, rows * width, width)
    high = lax.reduce_precision(flat, 8, 7)
    isometry = jnp.concatenate([high, high, flat - high], axis=2).astype(BF16)
    own = tensor
    scales = []
    for section in range(sections):
        own, largest, peak = level(
            own, isometry, section, parts, section > 0, section + 1 == sections
        )
        scales.append(largest)
    for shift in range(1, parts):
        if parts == 4:
            pairs = [(i, i ^ shift) for i in range(parts)]
        else:
            pairs = [(i, (i + shift) % parts) for i in range(parts)]
        scales.append(lax.ppermute(peak, "bond", pairs))
    final, log_density = pl.pallas_call(
        functools.partial(finish_kernel, sections),
        out_shape=[
            jax.ShapeDtypeStruct(own.shape, F32),
            jax.ShapeDtypeStruct((8, LANES), F32),
        ],
        name="finish",
    )(own, peak, *scales[1:])
    return final, log_density[0, :1]


def solution(mesh):
    in_specs = (P(("temp", "bond"), None), P("temp", "bond", None))
    out_specs = (P(("temp", "bond"), None), P("temp"))
    return jax.shard_map(
        on_device, mesh=mesh, in_specs=in_specs, out_specs=out_specs, check_vma=False
    )
```

```python
import functools

import jax
import jax.numpy as jnp
from jax import lax
from jax.experimental import pallas as pl
from jax.experimental.pallas import tpu as pltpu
from jax.sharding import PartitionSpec as P


EPSILON = 1e-06
LANES = 128
PITCH = 72
BF16 = jnp.bfloat16
F32 = jnp.float32


def split_isometry(rows, width, u_ref, spread):
    low_half = lax.broadcasted_iota(jnp.int32, (rows, LANES), 1) < width
    for x in range(width // 2):
        value = u_ref[:, x * LANES : (x + 1) * LANES]
        high = value.astype(BF16).astype(F32)
        low = value - high
        turned = pltpu.roll(high, width, 1)
        for at, highs, lows in (
            (2 * x, jnp.where(low_half, high, turned), low),
            (2 * x + 1, jnp.where(low_half, turned, high), pltpu.roll(low, width, 1)),
        ):
            spread[pl.ds(at, rows, stride=PITCH), :] = highs
            spread[pl.ds(rows * PITCH + at, rows, stride=PITCH), :] = lows


def contract(rows, width, wired, stacked, factor, u_ref, out_ref, placed, spread):
    split_isometry(rows, width, u_ref, spread)
    pairs = width // 2
    groups = pairs // 4
    cells = width * width
    low_half = lax.broadcasted_iota(jnp.int32, (pairs, LANES), 1) < width

    def first(q, g):
        blocks = []
        for n in range(4):
            at = pl.multiple_of((4 * q + n) * PITCH, 8)
            highs = spread[pl.ds(at, width), :]
            lows = spread[pl.ds(rows * PITCH + at, width), :]
            blocks.append(jnp.concatenate([highs, lows[:, :width]], axis=1))
        u = jnp.concatenate(blocks, axis=0).astype(BF16)
        return jnp.dot(u, stacked[:, g * 512 : (g + 1) * 512], preferred_element_type=F32)

    def second(inner, g):
        high = inner.astype(BF16)
        low = (inner - high.astype(F32)).astype(BF16)

        def block(array, i):
            return jnp.concatenate(
                [array[n * width : (n + 1) * width, i * LANES : (i + 1) * LANES] for n in range(4)],
                axis=1,
            )

        highs = [block(high, i) for i in range(4)]
        lows = [block(low, i) for i in range(4)]
        weights = jnp.concatenate([h for h in highs for _ in range(2)] + lows, axis=0)
        return jnp.dot(
            factor[:, g * 768 : (g + 1) * 768], weights, preferred_element_type=F32
        )

    def finish_quad(q, total, peak):
        for n in range(4):
            part = total[:, n * LANES : (n + 1) * LANES]
            even0, odd0, even1, odd1 = (part[r * pairs : (r + 1) * pairs] for r in range(4))
            kept = jnp.where(low_half, even0, odd1)
            moved = jnp.where(low_half, odd0, even1)
            value = kept + pltpu.roll(moved, width, 1)
            peak = jnp.maximum(peak, jnp.abs(value))
            at = (q // 2) * (8 * pairs) + (q % 2) * 4 + n
            placed[pl.ds(at, pairs, stride=8), :] = value
        return peak

    def several(count, start, peak):
        steps = [(start + r, g) for r in range(count) for g in range(groups)]
        total = None
        inner = first(*steps[0])
        for k, (q, g) in enumerate(steps):
            ahead = first(*steps[k + 1]) if k + 1 < len(steps) else None
            update = second(inner, g)
            total = update if g == 0 else total + update
            if g + 1 == groups:
                peak = finish_quad(q, total, peak)
            inner = ahead
        return peak

    peak = jnp.zeros((pairs, LANES), F32)
    quads = rows // 4
    each = 2 if quads % 2 == 0 else 1
    peak = lax.fori_loop(0, quads // each, lambda i, p: several(each, i * each, p), peak)
    highest = jnp.max(peak)
    tall = min(rows, 8)
    for h in range(rows // tall):
        for x in range(pairs):
            at = (h * pairs + x) * 8
            out_ref[h * tall : (h + 1) * tall, x * LANES : (x + 1) * LANES] = placed[at : at + tall, :]
    if wired:
        out_ref[:, cells:] = jnp.full((rows, LANES), highest, F32)
    return highest


def level_kernel(count, scaled, section, wired, rows, width, sources, *refs):
    pieces = refs[:count]
    u_ref, before_ref, out_ref, notes_ref, stacked, factor = refs[count : count + 6]
    whole, turned, placed, spread = refs[count + 6 :]
    held = pieces[0].shape[0]
    pairs = width // 2
    cells = width * width
    found = sources(lax.axis_index("bond"))
    log_density = before_ref[4:8, :]
    inverse = None
    if scaled:
        largest = jnp.max(pieces[0][:, cells:])
        for piece in pieces[1:]:
            largest = jnp.maximum(largest, jnp.max(piece[:, cells:]))
        largest = jnp.full((4, LANES), largest, F32) + EPSILON
        log_density = log_density + jnp.log(largest) * 0.5**section
        inverse = (1.0 / largest)[0:1, :]
    for j in range(count):
        start = pl.multiple_of(found[j] * held, 8)
        for x in range(pairs):
            value = pieces[j][:, x * LANES : (x + 1) * LANES]
            if scaled:
                value = value * inverse
            whole[pl.ds(start, held), x * LANES : (x + 1) * LANES] = value

    for x in range(pairs):
        lanes = slice(x * LANES, (x + 1) * LANES)
        value = whole[:, lanes]
        high = value.astype(BF16)
        high_wide = high.astype(F32)
        low = (value - high_wide).astype(BF16)
        stacked[0:width, lanes] = high
        stacked[width : 2 * width, lanes] = low
        stacked[2 * width : 3 * width, lanes] = high
        both = jnp.concatenate([high_wide, low.astype(F32)], axis=0).T
        turned[pl.ds(x, width, stride=PITCH), :] = both[:width]
        turned[pl.ds(pairs + x, width, stride=PITCH), :] = both[width:]

    groups = pairs // 4
    for g in range(groups):
        blocks = []
        for i in range(4):
            b = 2 * (4 * g + i)
            upper = turned[b * PITCH : b * PITCH + width, :].astype(BF16)
            lower = turned[(b + 1) * PITCH : (b + 1) * PITCH + width, :].astype(BF16)
            blocks.append(jnp.concatenate([upper, lower], axis=0))
        highs = [
            jnp.concatenate([blocks[i][:, :width], blocks[i + 1][:, :width]], axis=1)
            for i in (0, 2)
        ]
        factor[:, g * 768 : (g + 1) * 768] = jnp.concatenate(blocks + highs, axis=1)

    highest = contract(rows, width, wired, stacked, factor, u_ref, out_ref, placed, spread)
    notes_ref[0:4, :] = jnp.full((4, LANES), highest, F32)
    notes_ref[4:8, :] = log_density


def more_kernel(wired, rows, width, stacked, factor, u_ref, before_ref, out_ref, notes_ref, placed, spread):
    highest = contract(rows, width, wired, stacked, factor, u_ref, out_ref, placed, spread)
    notes_ref[0:4, :] = jnp.maximum(before_ref[0:4, :], highest)
    notes_ref[4:8, :] = before_ref[4:8, :]


def cost(rows, width):
    products = 2 * rows * width**4
    return pl.CostEstimate(flops=6 * products, bytes_accessed=16 * width**3, transcendentals=0)


def params():
    return pltpu.CompilerParams(vmem_limit_bytes=32 * 1024 * 1024)


def level(pieces, sources, isometry, notes, section, wired):
    width = sum(piece.shape[0] for piece in pieces)
    rows, cells = isometry.shape
    span = cells + LANES if wired else cells
    return pl.pallas_call(
        functools.partial(
            level_kernel, len(pieces), section > 0, section, wired, rows, width, sources
        ),
        out_shape=[
            jax.ShapeDtypeStruct((rows, span), F32),
            jax.ShapeDtypeStruct((8, LANES), F32),
            jax.ShapeDtypeStruct((3 * width, cells), BF16),
            jax.ShapeDtypeStruct((2 * width, 96 * width), BF16),
        ],
        scratch_shapes=[
            pltpu.VMEM((width, cells), F32),
            pltpu.VMEM((width * PITCH, LANES), F32),
            pltpu.VMEM((max(rows, 8) * width // 2, LANES), F32),
            pltpu.VMEM((2 * rows * PITCH, LANES), F32),
        ],
        compiler_params=params(),
        cost_estimate=cost(rows, width),
        name="level",
    )(*pieces, isometry, notes)


def more(stacked, factor, isometry, notes, wired):
    width = stacked.shape[0] // 3
    rows, cells = isometry.shape
    span = cells + LANES if wired else cells
    return pl.pallas_call(
        functools.partial(more_kernel, wired, rows, width),
        out_shape=[
            jax.ShapeDtypeStruct((rows, span), F32),
            jax.ShapeDtypeStruct((8, LANES), F32),
        ],
        scratch_shapes=[
            pltpu.VMEM((max(rows, 8) * width // 2, LANES), F32),
            pltpu.VMEM((2 * rows * PITCH, LANES), F32),
        ],
        compiler_params=params(),
        cost_estimate=cost(rows, width),
        name="more",
    )(stacked, factor, isometry, notes)


def middle_sources(me):
    return [me, me ^ 1, me ^ 3, me ^ 2]


def on_line(tensor, isometries):
    sections = isometries.shape[0]
    send = lambda x, pairs: lax.ppermute(x, "bond", pairs)
    inward, swap, outward = [(0, 1), (3, 2)], [(1, 2), (2, 1)], [(1, 0), (2, 3)]
    far = send(tensor, [(0, 2), (3, 1)])
    near = send(tensor, inward)
    other = send(tensor, swap)
    pieces = [tensor, near, other, far]
    theirs = [send(isometries[0], inward)]
    later = send(isometries[1:], inward)
    theirs += [later[k] for k in range(sections - 1)]
    notes = jnp.zeros((8, LANES), F32)
    for section in range(sections):
        last = section + 1 == sections
        mine = isometries[section]
        order = [theirs[section], mine] if last else [mine, theirs[section]]
        first, notes, stacked, factor = level(
            pieces, middle_sources, order[0], notes, section, not last
        )
        if last:
            break
        first_other = send(first, swap)
        second, notes = more(stacked, factor, order[1], notes, True)
        second_other = send(second, swap)
        pieces = [first, second, first_other, second_other]
    moved = send(first, outward)
    second, notes = more(stacked, factor, order[1], notes, False)
    found = [notes, send(notes, swap), send(notes, outward), send(notes, [(1, 3), (2, 0)])]
    return pl.pallas_call(
        functools.partial(line_finish_kernel, sections),
        out_shape=[
            jax.ShapeDtypeStruct(tensor.shape, F32),
            jax.ShapeDtypeStruct((8, LANES), F32),
        ],
        compiler_params=params(),
        name="finish",
    )(second, moved, *found)


def line_finish_kernel(sections, second_ref, moved_ref, own, swapped, near, far, out_ref, log_ref):
    me = lax.axis_index("bond")
    inner = jnp.logical_or(me == 1, me == 2)

    def write(value_ref, one, two):
        largest = jnp.maximum(one[0:4, :], two[0:4, :]) + EPSILON
        log_density = one[4:8, :] + jnp.log(largest) * 0.5**sections
        log_ref[0:4, :] = log_density
        log_ref[4:8, :] = log_density
        out_ref[...] = value_ref[...] / largest[0:1, 0:1]

    @pl.when(inner)
    def _():
        write(second_ref, own, swapped)

    @pl.when(jnp.logical_not(inner))
    def _():
        write(moved_ref, near, far)


def gathered(tensor, isometries):
    sections = isometries.shape[0]
    own = tensor
    notes = jnp.zeros((8, LANES), F32)
    for section in range(sections):
        piece = lax.all_gather(own, "bond", axis=0, tiled=True)
        own, notes, _, _ = level(
            [piece],
            lambda me: [0],
            isometries[section],
            notes,
            section,
            section + 1 < sections,
        )
    largest = lax.pmax(notes[0, :1], "bond") + EPSILON
    return own / largest[0], notes[4, :1] + jnp.log(largest) * 0.5**sections


def on_device(tensor, isometries):
    if lax.axis_size("bond") == 4:
        final, log_density = on_line(tensor, isometries)
        return final, log_density[0, :1]
    return gathered(tensor, isometries)


def solution(mesh):
    in_specs = (P(("temp", "bond"), None), P("temp", "bond", None))
    out_specs = (P(("temp", "bond"), None), P("temp"))
    return jax.shard_map(
        on_device, mesh=mesh, in_specs=in_specs, out_specs=out_specs, check_vma=False
    )
```

```python
import functools

import jax
import jax.numpy as jnp
from jax import lax
from jax.experimental import pallas as pl
from jax.experimental.pallas import tpu as pltpu
from jax.sharding import PartitionSpec as P


EPSILON = 1e-06
LANES = 128
PITCH = 72
BF16 = jnp.bfloat16
F32 = jnp.float32


def split_isometry(rows, width, u_ref, spread):
    low_half = lax.broadcasted_iota(jnp.int32, (rows, LANES), 1) < width
    for x in range(width // 2):
        value = u_ref[:, x * LANES : (x + 1) * LANES]
        high = value.astype(BF16).astype(F32)
        low = value - high
        turned = pltpu.roll(high, width, 1)
        for at, highs, lows in (
            (2 * x, jnp.where(low_half, high, turned), low),
            (2 * x + 1, jnp.where(low_half, turned, high), pltpu.roll(low, width, 1)),
        ):
            spread[pl.ds(at, rows, stride=PITCH), :] = highs
            spread[pl.ds(rows * PITCH + at, rows, stride=PITCH), :] = lows


def contract(rows, width, wired, stacked, factor, u_ref, out_ref, placed, spread):
    split_isometry(rows, width, u_ref, spread)
    pairs = width // 2
    groups = pairs // 4
    cells = width * width
    batch = min(rows, 8)
    low_half = lax.broadcasted_iota(jnp.int32, (width, LANES), 1) < width
    low_few = lax.broadcasted_iota(jnp.int32, (pairs, LANES), 1) < width

    def first(q, g):
        blocks = []
        for n in range(batch):
            at = pl.multiple_of((batch * q + n) * PITCH, 8)
            highs = spread[pl.ds(at, width), :]
            lows = spread[pl.ds(rows * PITCH + at, width), :]
            blocks.append(jnp.concatenate([highs, lows[:, :width]], axis=1))
        u = jnp.concatenate(blocks, axis=0).astype(BF16)
        return jnp.dot(u, stacked[:, g * 512 : (g + 1) * 512], preferred_element_type=F32)

    def second(inner, g):
        strips = []
        for i in range(4):
            evens, odds = [], []
            for n in range(0, batch, 2):
                lanes = slice(i * LANES, (i + 1) * LANES)
                one = inner[n * width : (n + 1) * width, lanes]
                two = inner[(n + 1) * width : (n + 2) * width, lanes]
                kept = jnp.where(low_half, one, two)
                moved = pltpu.roll(jnp.where(low_half, two, one), width, 1)
                evens.append(jnp.where(low_half, kept, moved))
                odds.append(jnp.where(low_half, moved, kept))
            strips += [jnp.concatenate(evens, axis=1), jnp.concatenate(odds, axis=1)]
        weights = jnp.concatenate(strips, axis=0)
        high = weights.astype(BF16)
        low = (weights - high.astype(F32)).astype(BF16)
        left = factor[:, g * 512 : (g + 1) * 512]
        return (
            jnp.dot(left, high, preferred_element_type=F32),
            jnp.dot(left[:width], low, preferred_element_type=F32),
        )

    def finish_batch(q, total, peak):
        total = total[0][:width] + (total[0][width:] + total[1])
        for n in range(0, batch, 2):
            part = total[:, n // 2 * LANES : (n // 2 + 1) * LANES]
            even, odd = part[:pairs], part[pairs:]
            for r, value in (
                (n, jnp.where(low_few, even, pltpu.roll(odd, width, 1))),
                (n + 1, jnp.where(low_few, pltpu.roll(even, width, 1), odd)),
            ):
                peak = jnp.maximum(peak, jnp.abs(value))
                placed[pl.ds(q * (8 * pairs) + r, pairs, stride=8), :] = value
        return peak

    def several(count, start, peak):
        steps = [(start + r, g) for r in range(count) for g in range(groups)]
        total = None
        inner = first(*steps[0])
        for k, (q, g) in enumerate(steps):
            ahead = first(*steps[k + 1]) if k + 1 < len(steps) else None
            update = second(inner, g)
            total = update if g == 0 else (total[0] + update[0], total[1] + update[1])
            if g + 1 == groups:
                peak = finish_batch(q, total, peak)
            inner = ahead
        return peak

    peak = jnp.zeros((pairs, LANES), F32)
    peak = lax.fori_loop(0, rows // batch, lambda i, p: several(1, i, p), peak)
    highest = jnp.max(peak)
    tall = min(rows, 8)
    for h in range(rows // tall):
        for x in range(pairs):
            at = (h * pairs + x) * 8
            out_ref[h * tall : (h + 1) * tall, x * LANES : (x + 1) * LANES] = placed[at : at + tall, :]
    if wired:
        out_ref[:, cells:] = jnp.full((rows, LANES), highest, F32)
    return highest


def level_kernel(count, scaled, section, wired, rows, width, sources, *refs):
    pieces = refs[:count]
    u_ref, before_ref, out_ref, notes_ref, stacked, factor = refs[count : count + 6]
    whole, turned, placed, spread = refs[count + 6 :]
    held = pieces[0].shape[0]
    pairs = width // 2
    cells = width * width
    found = sources(lax.axis_index("bond"))
    log_density = before_ref[4:8, :]
    inverse = None
    if scaled:
        largest = jnp.max(pieces[0][:, cells:])
        for piece in pieces[1:]:
            largest = jnp.maximum(largest, jnp.max(piece[:, cells:]))
        largest = jnp.full((4, LANES), largest, F32) + EPSILON
        log_density = log_density + jnp.log(largest) * 0.5**section
        inverse = (1.0 / largest)[0:1, :]
    for j in range(count):
        start = pl.multiple_of(found[j] * held, 8)
        for x in range(pairs):
            value = pieces[j][:, x * LANES : (x + 1) * LANES]
            if scaled:
                value = value * inverse
            whole[pl.ds(start, held), x * LANES : (x + 1) * LANES] = value

    for x in range(pairs):
        lanes = slice(x * LANES, (x + 1) * LANES)
        value = whole[:, lanes]
        high = value.astype(BF16)
        high_wide = high.astype(F32)
        low = (value - high_wide).astype(BF16)
        stacked[0:width, lanes] = high
        stacked[width : 2 * width, lanes] = low
        stacked[2 * width : 3 * width, lanes] = high
        both = jnp.concatenate([high_wide, low.astype(F32)], axis=0).T
        turned[pl.ds(x, width, stride=PITCH), :] = both[:width]
        turned[pl.ds(pairs + x, width, stride=PITCH), :] = both[width:]

    low_half = lax.broadcasted_iota(jnp.int32, (width, LANES), 1) < width
    for x in range(pairs):
        one = turned[2 * x * PITCH : 2 * x * PITCH + width, :]
        two = turned[(2 * x + 1) * PITCH : (2 * x + 1) * PITCH + width, :]
        lanes = slice(x * LANES, (x + 1) * LANES)
        kept = jnp.where(low_half, one, two)
        moved = pltpu.roll(jnp.where(low_half, two, one), width, 1)
        factor[0:width, lanes] = jnp.where(low_half, kept, moved).astype(BF16)
        factor[width:, lanes] = jnp.where(low_half, moved, kept).astype(BF16)

    highest = contract(rows, width, wired, stacked, factor, u_ref, out_ref, placed, spread)
    notes_ref[0:4, :] = jnp.full((4, LANES), highest, F32)
    notes_ref[4:8, :] = log_density


def more_kernel(wired, rows, width, stacked, factor, u_ref, before_ref, out_ref, notes_ref, placed, spread):
    highest = contract(rows, width, wired, stacked, factor, u_ref, out_ref, placed, spread)
    notes_ref[0:4, :] = jnp.maximum(before_ref[0:4, :], highest)
    notes_ref[4:8, :] = before_ref[4:8, :]


def cost(rows, width):
    products = 2 * rows * width**4
    return pl.CostEstimate(flops=6 * products, bytes_accessed=16 * width**3, transcendentals=0)


def params():
    return pltpu.CompilerParams(vmem_limit_bytes=32 * 1024 * 1024)


def level(pieces, sources, isometry, notes, section, wired):
    width = sum(piece.shape[0] for piece in pieces)
    rows, cells = isometry.shape
    span = cells + LANES if wired else cells
    return pl.pallas_call(
        functools.partial(
            level_kernel, len(pieces), section > 0, section, wired, rows, width, sources
        ),
        out_shape=[
            jax.ShapeDtypeStruct((rows, span), F32),
            jax.ShapeDtypeStruct((8, LANES), F32),
            jax.ShapeDtypeStruct((3 * width, cells), BF16),
            jax.ShapeDtypeStruct((2 * width, cells), BF16),
        ],
        scratch_shapes=[
            pltpu.VMEM((width, cells), F32),
            pltpu.VMEM((width * PITCH, LANES), F32),
            pltpu.VMEM((max(rows, 8) * width // 2, LANES), F32),
            pltpu.VMEM((2 * rows * PITCH, LANES), F32),
        ],
        compiler_params=params(),
        cost_estimate=cost(rows, width),
        name="level",
    )(*pieces, isometry, notes)


def more(stacked, factor, isometry, notes, wired):
    width = stacked.shape[0] // 3
    rows, cells = isometry.shape
    span = cells + LANES if wired else cells
    return pl.pallas_call(
        functools.partial(more_kernel, wired, rows, width),
        out_shape=[
            jax.ShapeDtypeStruct((rows, span), F32),
            jax.ShapeDtypeStruct((8, LANES), F32),
        ],
        scratch_shapes=[
            pltpu.VMEM((max(rows, 8) * width // 2, LANES), F32),
            pltpu.VMEM((2 * rows * PITCH, LANES), F32),
        ],
        compiler_params=params(),
        cost_estimate=cost(rows, width),
        name="more",
    )(stacked, factor, isometry, notes)


def middle_sources(me):
    return [me, me ^ 1, me ^ 3, me ^ 2]


def on_line(tensor, isometries):
    sections = isometries.shape[0]
    send = lambda x, pairs: lax.ppermute(x, "bond", pairs)
    inward, swap, outward = [(0, 1), (3, 2)], [(1, 2), (2, 1)], [(1, 0), (2, 3)]
    near = send(tensor, inward)
    far = send(tensor, [(0, 2), (3, 1)])
    other = send(tensor, swap)
    pieces = [tensor, near, other, far]
    theirs = [send(isometries[0], inward)]
    later = send(isometries[1:], inward)
    theirs += [later[k] for k in range(sections - 1)]
    notes = jnp.zeros((8, LANES), F32)
    for section in range(sections):
        last = section + 1 == sections
        mine = isometries[section]
        order = [theirs[section], mine] if last else [mine, theirs[section]]
        first, notes, stacked, factor = level(
            pieces, middle_sources, order[0], notes, section, not last
        )
        if last:
            break
        first_other = send(first, swap)
        second, notes = more(stacked, factor, order[1], notes, True)
        second_other = send(second, swap)
        pieces = [first, second, first_other, second_other]
    moved = send(first, outward)
    second, notes = more(stacked, factor, order[1], notes, False)
    found = [notes, send(notes, swap), send(notes, outward), send(notes, [(1, 3), (2, 0)])]
    return pl.pallas_call(
        functools.partial(line_finish_kernel, sections),
        out_shape=[
            jax.ShapeDtypeStruct(tensor.shape, F32),
            jax.ShapeDtypeStruct((1, 1), F32),
        ],
        out_specs=[
            pl.BlockSpec(memory_space=pltpu.VMEM),
            pl.BlockSpec(memory_space=pltpu.SMEM),
        ],
        compiler_params=params(),
        name="finish",
    )(second, moved, *found)


def line_finish_kernel(sections, second_ref, moved_ref, own, swapped, near, far, out_ref, log_ref):
    me = lax.axis_index("bond")
    inner = jnp.logical_or(me == 1, me == 2)

    def write(value_ref, one, two):
        largest = jnp.maximum(one[0:4, :], two[0:4, :]) + EPSILON
        log_density = one[4:8, :] + jnp.log(largest) * 0.5**sections
        log_ref[0, 0] = jnp.max(log_density)
        out_ref[...] = value_ref[...] / largest[0:1, 0:1]

    @pl.when(inner)
    def _():
        write(second_ref, own, swapped)

    @pl.when(jnp.logical_not(inner))
    def _():
        write(moved_ref, near, far)


def gathered(tensor, isometries):
    sections = isometries.shape[0]
    own = tensor
    notes = jnp.zeros((8, LANES), F32)
    for section in range(sections):
        piece = lax.all_gather(own, "bond", axis=0, tiled=True)
        own, notes, _, _ = level(
            [piece],
            lambda me: [0],
            isometries[section],
            notes,
            section,
            section + 1 < sections,
        )
    largest = lax.pmax(notes[0, :1], "bond") + EPSILON
    return own / largest[0], notes[4, :1] + jnp.log(largest) * 0.5**sections


def on_device(tensor, isometries):
    if lax.axis_size("bond") == 4:
        final, log_density = on_line(tensor, isometries)
        return final, log_density.reshape(1)
    return gathered(tensor, isometries)


def solution(mesh):
    in_specs = (P(("temp", "bond"), None), P("temp", "bond", None))
    out_specs = (P(("temp", "bond"), None), P("temp"))
    return jax.shard_map(
        on_device, mesh=mesh, in_specs=in_specs, out_specs=out_specs, check_vma=False
    )
```

```python
import functools

import jax
import jax.numpy as jnp
from jax import lax
from jax.experimental import pallas as pl
from jax.experimental.pallas import tpu as pltpu
from jax.sharding import PartitionSpec as P


EPSILON = 1e-06
LANES = 128
PITCH = 72
BF16 = jnp.bfloat16
F32 = jnp.float32


def split_isometry(rows, width, u_ref, spread):
    low_half = lax.broadcasted_iota(jnp.int32, (rows, LANES), 1) < width
    for x in range(width // 2):
        value = u_ref[:, x * LANES : (x + 1) * LANES]
        high = value.astype(BF16).astype(F32)
        low = value - high
        turned = pltpu.roll(high, width, 1)
        for at, highs, lows in (
            (2 * x, jnp.where(low_half, high, turned), low),
            (2 * x + 1, jnp.where(low_half, turned, high), pltpu.roll(low, width, 1)),
        ):
            spread[pl.ds(at, rows, stride=PITCH), :] = highs
            spread[pl.ds(rows * PITCH + at, rows, stride=PITCH), :] = lows


def contract(rows, width, wired, stacked, factor, u_ref, out_ref, placed, spread):
    split_isometry(rows, width, u_ref, spread)
    pairs = width // 2
    groups = pairs // 4
    cells = width * width
    batch = min(rows, 8)
    low_half = lax.broadcasted_iota(jnp.int32, (width, LANES), 1) < width
    low_few = lax.broadcasted_iota(jnp.int32, (pairs, LANES), 1) < width

    def first(q, g):
        blocks = []
        for n in range(batch):
            at = pl.multiple_of((batch * q + n) * PITCH, 8)
            highs = spread[pl.ds(at, width), :]
            lows = spread[pl.ds(rows * PITCH + at, width), :]
            blocks.append(jnp.concatenate([highs, lows[:, :width]], axis=1))
        u = jnp.concatenate(blocks, axis=0).astype(BF16)
        return jnp.dot(u, stacked[:, g * 512 : (g + 1) * 512], preferred_element_type=F32)

    def second(inner, g):
        strips = []
        for i in range(4):
            evens, odds = [], []
            for n in range(0, batch, 2):
                lanes = slice(i * LANES, (i + 1) * LANES)
                one = inner[n * width : (n + 1) * width, lanes]
                two = inner[(n + 1) * width : (n + 2) * width, lanes]
                kept = jnp.where(low_half, one, two)
                moved = pltpu.roll(jnp.where(low_half, two, one), width, 1)
                evens.append(jnp.where(low_half, kept, moved))
                odds.append(jnp.where(low_half, moved, kept))
            strips += [jnp.concatenate(evens, axis=1), jnp.concatenate(odds, axis=1)]
        weights = jnp.concatenate(strips, axis=0)
        high = weights.astype(BF16)
        low = (weights - high.astype(F32)).astype(BF16)
        left = factor[:, g * 512 : (g + 1) * 512]
        return (
            jnp.dot(left, high, preferred_element_type=F32),
            jnp.dot(left[:width], low, preferred_element_type=F32),
        )

    def finish_batch(q, total, peak):
        total = total[0][:width] + (total[0][width:] + total[1])
        for n in range(0, batch, 2):
            part = total[:, n // 2 * LANES : (n // 2 + 1) * LANES]
            even, odd = part[:pairs], part[pairs:]
            for r, value in (
                (n, jnp.where(low_few, even, pltpu.roll(odd, width, 1))),
                (n + 1, jnp.where(low_few, pltpu.roll(even, width, 1), odd)),
            ):
                peak = jnp.maximum(peak, jnp.abs(value))
                placed[pl.ds(q * (8 * pairs) + r, pairs, stride=8), :] = value
        return peak

    def several(count, start, peak):
        steps = [(start + r, g) for r in range(count) for g in range(groups)]
        total = None
        inner = first(*steps[0])
        for k, (q, g) in enumerate(steps):
            ahead = first(*steps[k + 1]) if k + 1 < len(steps) else None
            update = second(inner, g)
            total = update if g == 0 else (total[0] + update[0], total[1] + update[1])
            if g + 1 == groups:
                peak = finish_batch(q, total, peak)
            inner = ahead
        return peak

    peak = jnp.zeros((pairs, LANES), F32)
    peak = lax.fori_loop(0, rows // batch, lambda i, p: several(1, i, p), peak)
    highest = jnp.max(peak)
    tall = min(rows, 8)
    for h in range(rows // tall):
        for x in range(pairs):
            at = (h * pairs + x) * 8
            out_ref[h * tall : (h + 1) * tall, x * LANES : (x + 1) * LANES] = placed[at : at + tall, :]
    if wired:
        out_ref[:, cells:] = jnp.full((rows, LANES), highest, F32)
    return highest


def split_tensor(
    pieces, scaled, section, width, sources, before_ref, notes_ref, stacked, factor, whole, turned
):
    held = pieces[0].shape[0]
    pairs = width // 2
    cells = width * width
    count = len(pieces)
    found = sources(lax.axis_index("bond"))
    log_density = before_ref[4:8, :]
    inverse = None
    if scaled:
        largest = jnp.max(pieces[0][:, cells:])
        for piece in pieces[1:]:
            largest = jnp.maximum(largest, jnp.max(piece[:, cells:]))
        largest = jnp.full((4, LANES), largest, F32) + EPSILON
        log_density = log_density + jnp.log(largest) * 0.5**section
        inverse = (1.0 / largest)[0:1, :]
    for j in range(count):
        start = pl.multiple_of(found[j] * held, 8)
        for x in range(pairs):
            value = pieces[j][:, x * LANES : (x + 1) * LANES]
            if scaled:
                value = value * inverse
            whole[pl.ds(start, held), x * LANES : (x + 1) * LANES] = value

    for x in range(pairs):
        lanes = slice(x * LANES, (x + 1) * LANES)
        value = whole[:, lanes]
        high = value.astype(BF16)
        high_wide = high.astype(F32)
        low = (value - high_wide).astype(BF16)
        stacked[0:width, lanes] = high
        stacked[width : 2 * width, lanes] = low
        stacked[2 * width : 3 * width, lanes] = high
        both = jnp.concatenate([high_wide, low.astype(F32)], axis=0).T
        turned[pl.ds(x, width, stride=PITCH), :] = both[:width]
        turned[pl.ds(pairs + x, width, stride=PITCH), :] = both[width:]

    low_half = lax.broadcasted_iota(jnp.int32, (width, LANES), 1) < width
    for x in range(pairs):
        one = turned[2 * x * PITCH : 2 * x * PITCH + width, :]
        two = turned[(2 * x + 1) * PITCH : (2 * x + 1) * PITCH + width, :]
        lanes = slice(x * LANES, (x + 1) * LANES)
        kept = jnp.where(low_half, one, two)
        moved = pltpu.roll(jnp.where(low_half, two, one), width, 1)
        factor[0:width, lanes] = jnp.where(low_half, kept, moved).astype(BF16)
        factor[width:, lanes] = jnp.where(low_half, moved, kept).astype(BF16)

    notes_ref[4:8, :] = log_density


def level_kernel(count, scaled, section, wired, rows, width, sources, *refs):
    pieces = refs[:count]
    u_ref, before_ref, out_ref, notes_ref, stacked, factor = refs[count : count + 6]
    whole, turned, placed, spread = refs[count + 6 :]
    split_tensor(
        pieces, scaled, section, width, sources, before_ref, notes_ref, stacked, factor, whole, turned
    )
    highest = contract(rows, width, wired, stacked, factor, u_ref, out_ref, placed, spread)
    notes_ref[0:4, :] = jnp.full((4, LANES), highest, F32)


def last_kernel(count, section, rows, width, sources, *refs):
    pieces = refs[:count]
    end_u_ref, u_ref, before_ref, end_out_ref, out_ref, notes_ref = refs[count : count + 6]
    stacked, factor, whole, turned, placed, spread = refs[count + 6 :]
    cells = width * width
    split_tensor(pieces, True, section, width, sources, before_ref, notes_ref, stacked, factor, whole, turned)
    one = contract(rows, width, False, stacked, factor, end_u_ref, end_out_ref, placed, spread)
    two = contract(rows, width, False, stacked, factor, u_ref, out_ref, placed, spread)
    notes_ref[0:4, :] = jnp.full((4, LANES), jnp.maximum(one, two), F32)
    end_out_ref[0:8, cells:] = notes_ref[...]


def more_kernel(wired, rows, width, stacked, factor, u_ref, before_ref, out_ref, notes_ref, placed, spread):
    highest = contract(rows, width, wired, stacked, factor, u_ref, out_ref, placed, spread)
    notes_ref[0:4, :] = jnp.maximum(before_ref[0:4, :], highest)
    notes_ref[4:8, :] = before_ref[4:8, :]


def cost(rows, width):
    products = 2 * rows * width**4
    return pl.CostEstimate(flops=6 * products, bytes_accessed=16 * width**3, transcendentals=0)


def params():
    return pltpu.CompilerParams(vmem_limit_bytes=32 * 1024 * 1024)


def level(pieces, sources, isometry, notes, section, wired):
    width = sum(piece.shape[0] for piece in pieces)
    rows, cells = isometry.shape
    span = cells + LANES if wired else cells
    return pl.pallas_call(
        functools.partial(
            level_kernel, len(pieces), section > 0, section, wired, rows, width, sources
        ),
        out_shape=[
            jax.ShapeDtypeStruct((rows, span), F32),
            jax.ShapeDtypeStruct((8, LANES), F32),
            jax.ShapeDtypeStruct((3 * width, cells), BF16),
            jax.ShapeDtypeStruct((2 * width, cells), BF16),
        ],
        scratch_shapes=[
            pltpu.VMEM((width, cells), F32),
            pltpu.VMEM((width * PITCH, LANES), F32),
            pltpu.VMEM((max(rows, 8) * width // 2, LANES), F32),
            pltpu.VMEM((2 * rows * PITCH, LANES), F32),
        ],
        compiler_params=params(),
        cost_estimate=cost(rows, width),
        name="level",
    )(*pieces, isometry, notes)


def last_level(pieces, sources, end_isometry, isometry, notes, section):
    width = sum(piece.shape[0] for piece in pieces)
    rows, cells = isometry.shape
    return pl.pallas_call(
        functools.partial(last_kernel, len(pieces), section, rows, width, sources),
        out_shape=[
            jax.ShapeDtypeStruct((rows, cells + LANES), F32),
            jax.ShapeDtypeStruct((rows, cells), F32),
            jax.ShapeDtypeStruct((8, LANES), F32),
        ],
        scratch_shapes=[
            pltpu.VMEM((3 * width, cells), BF16),
            pltpu.VMEM((2 * width, cells), BF16),
            pltpu.VMEM((width, cells), F32),
            pltpu.VMEM((width * PITCH, LANES), F32),
            pltpu.VMEM((max(rows, 8) * width // 2, LANES), F32),
            pltpu.VMEM((2 * rows * PITCH, LANES), F32),
        ],
        compiler_params=params(),
        cost_estimate=cost(2 * rows, width),
        name="last",
    )(*pieces, end_isometry, isometry, notes)


def more(stacked, factor, isometry, notes, wired):
    width = stacked.shape[0] // 3
    rows, cells = isometry.shape
    span = cells + LANES if wired else cells
    return pl.pallas_call(
        functools.partial(more_kernel, wired, rows, width),
        out_shape=[
            jax.ShapeDtypeStruct((rows, span), F32),
            jax.ShapeDtypeStruct((8, LANES), F32),
        ],
        scratch_shapes=[
            pltpu.VMEM((max(rows, 8) * width // 2, LANES), F32),
            pltpu.VMEM((2 * rows * PITCH, LANES), F32),
        ],
        compiler_params=params(),
        cost_estimate=cost(rows, width),
        name="more",
    )(stacked, factor, isometry, notes)


def middle_sources(me):
    return [me, me ^ 1, me ^ 3, me ^ 2]


def on_line(tensor, isometries):
    sections = isometries.shape[0]
    send = lambda x, pairs: lax.ppermute(x, "bond", pairs)
    inward, swap, outward = [(0, 1), (3, 2)], [(1, 2), (2, 1)], [(1, 0), (2, 3)]
    near = send(tensor, inward)
    far = send(tensor, [(0, 2), (3, 1)])
    other = send(tensor, swap)
    pieces = [tensor, near, other, far]
    theirs = [send(isometries[0], inward)]
    later = send(isometries[1:], inward)
    theirs += [later[k] for k in range(sections - 1)]
    notes = jnp.zeros((8, LANES), F32)
    for section in range(sections - 1):
        first, notes, stacked, factor = level(
            pieces, middle_sources, isometries[section], notes, section, True
        )
        first_other = send(first, swap)
        second, notes = more(stacked, factor, theirs[section], notes, True)
        second_other = send(second, swap)
        pieces = [first, second, first_other, second_other]
    moved, own, notes = last_level(
        pieces, middle_sources, theirs[-1], isometries[sections - 1], notes, sections - 1
    )
    moved = send(moved, outward)
    across = send(notes, [(1, 3), (2, 0)])
    swapped = send(notes, swap)
    return pl.pallas_call(
        functools.partial(line_finish_kernel, sections),
        out_shape=[
            jax.ShapeDtypeStruct(tensor.shape, F32),
            jax.ShapeDtypeStruct((1, 1), F32),
        ],
        out_specs=[
            pl.BlockSpec(memory_space=pltpu.VMEM),
            pl.BlockSpec(memory_space=pltpu.SMEM),
        ],
        compiler_params=params(),
        name="finish",
    )(own, moved, notes, swapped, across)


def line_finish_kernel(sections, own_ref, moved_ref, notes, swapped, across, out_ref, log_ref):
    me = lax.axis_index("bond")
    inner = jnp.logical_or(me == 1, me == 2)
    cells = own_ref.shape[1]

    def write(value_ref, one, two):
        largest = jnp.maximum(one[0:4, :], two[0:4, :]) + EPSILON
        log_ref[0, 0] = jnp.max(one[4:8, :] + jnp.log(largest) * 0.5**sections)
        out_ref[...] = value_ref[:, :cells] / largest[0:1, 0:1]

    @pl.when(inner)
    def _():
        write(own_ref, notes[...], swapped)

    @pl.when(jnp.logical_not(inner))
    def _():
        write(moved_ref, moved_ref[0:8, cells:], across)


def gathered(tensor, isometries):
    sections = isometries.shape[0]
    own = tensor
    notes = jnp.zeros((8, LANES), F32)
    for section in range(sections):
        piece = lax.all_gather(own, "bond", axis=0, tiled=True)
        own, notes, _, _ = level(
            [piece],
            lambda me: [0],
            isometries[section],
            notes,
            section,
            section + 1 < sections,
        )
    largest = lax.pmax(notes[0, :1], "bond") + EPSILON
    return own / largest[0], notes[4, :1] + jnp.log(largest) * 0.5**sections


def on_device(tensor, isometries):
    if lax.axis_size("bond") == 4:
        final, log_density = on_line(tensor, isometries)
        return final, log_density.reshape(1)
    return gathered(tensor, isometries)


def solution(mesh):
    in_specs = (P(("temp", "bond"), None), P("temp", "bond", None))
    out_specs = (P(("temp", "bond"), None), P("temp"))
    return jax.shard_map(
        on_device, mesh=mesh, in_specs=in_specs, out_specs=out_specs, check_vma=False
    )
```
